32 devices in a mesh: rep: 1, r: 4 (over z), s: 8 (over x, y, core).
Axes of the slice: x: 2, y: 2, z: 4, core: 2. Of those that a mesh axis runs over, the one named last changes fastest.
Arguments:
- x: bfloat16 [32, 4096, 512], P(('rep', 'r', 's'))
- dy: bfloat16 [32, 4096, 512], P(('rep', 'r', 's'))
- w_gate: bfloat16 [2, 512, 4096], P(None, 's')
- w_up: bfloat16 [2, 512, 4096], P(None, 's')
- w_down: bfloat16 [2, 4096, 512], P(None, 's')
- m_w_gate: float32 [2, 512, 4096], P(None, 's')
- m_w_up: float32 [2, 512, 4096], P(None, 's')
- m_w_down: float32 [2, 4096, 512], P(None, 's')
- v_w_gate: float32 [2, 512, 4096], P(None, 's')
- v_w_up: float32 [2, 512, 4096], P(None, 's')
- v_w_down: float32 [2, 4096, 512], P(None, 's')
Outputs:
- output 1: bfloat16 [2, 512, 4096], P('rep', 's')
- output 2: bfloat16 [2, 512, 4096], P('rep', 's')
- output 3: bfloat16 [2, 4096, 512], P('rep', 's')
- output 4: float32 [2, 512, 4096], P('rep', 's')
- output 5: float32 [2, 512, 4096], P('rep', 's')
- output 6: float32 [2, 4096, 512], P('rep', 's')
- output 7: float32 [2, 512, 4096], P('rep', 's')
- output 8: float32 [2, 512, 4096], P('rep', 's')
- output 9: float32 [2, 4096, 512], P('rep', 's')
All inputs are finite; a program needn't handle non-finite values.
Results may differ from the reference program's by a relative error of at most 0.022.
Values are sent between devices in bfloat16 or wider.
A program may use at most 2 GiB of HBM per device.

```python
import jax
import jax.numpy as jnp
from jax import lax

SEQUENCES = 32
TOKENS = 4096
D = 512
FF = 4096
LAYERS = 2
NAMES = ("w_gate", "w_up", "w_down")
SHAPES = {"w_gate": (LAYERS, D, FF), "w_up": (LAYERS, D, FF), "w_down": (LAYERS, FF, D)}


def bump(key, n, height):
    away = (jnp.arange(n, dtype=jnp.int32) - jax.random.randint(key, (), 0, n, jnp.int32)) % n
    return jnp.where(away < n // 8, height, 1.0)


def together(key, own, strength):
    shared = jax.random.normal(key, own.shape[1:], jnp.float32)
    return (own + strength * shared) * lax.rsqrt(1 + strength * strength)


def setup_inputs(seed: int = 0, part: int = 0) -> dict:
    kx, kdy, ka, kb, kz, kf, kh, kl, *keys = jax.random.split(jax.random.key(seed), 8 + 3 * len(NAMES))
    kx, kdy, ka, kb = (jax.random.fold_in(k, part) for k in (kx, kdy, ka, kb))
    kw, km, kv = (keys[i::3] for i in range(3))
    shape = (SEQUENCES, TOKENS, D)
    much_x, much_dy = jax.random.uniform(kz, (2,), jnp.float32, 0.0, 1.0)
    loud = 2.0 ** jax.random.uniform(jax.random.fold_in(kz, 1), (), jnp.float32, -1.0, 2.0)
    layers = 2.0 ** jax.random.uniform(kl, (LAYERS, 1, 1), jnp.float32, -1.0, 1.0)
    x = together(ka, jax.random.normal(kx, shape, jnp.float32), much_x) * bump(kf, D, 4.0)
    dy = together(kb, jax.random.normal(kdy, shape, jnp.float32), much_dy)
    drawn = {"x": x.astype(jnp.bfloat16), "dy": (loud * dy * (SEQUENCES * TOKENS) ** -0.5).astype(jnp.bfloat16)}
    for key, name in zip(kw, NAMES, strict=True):
        w = jax.random.normal(key, SHAPES[name], jnp.float32) * SHAPES[name][1] ** -0.5
        drawn[name] = (w * {"w_gate": 1.0, "w_up": bump(kh, FF, 4.0), "w_down": layers}[name]).astype(jnp.bfloat16)
    for key, name in zip(km, NAMES, strict=True):
        drawn[f"m_{name}"] = 0.1 * jax.random.normal(key, SHAPES[name], jnp.float32)
    for key, name in zip(kv, NAMES, strict=True):
        drawn[f"v_{name}"] = jax.random.uniform(key, SHAPES[name], jnp.float32, 0.005, 0.015)
    return drawn


def matmul(a, w):
    return jnp.dot(a, w, preferred_element_type=jnp.float32).astype(jnp.bfloat16)


def normed(h):
    wide = h.astype(jnp.float32)
    scale = lax.rsqrt(jnp.mean(wide**2, -1, keepdims=True) + 1e-6)
    return (wide * scale).astype(jnp.bfloat16)


def layer(h, w):
    a = normed(h)
    gate = jnp.dot(a, w["w_gate"], preferred_element_type=jnp.float32)
    up = jnp.dot(a, w["w_up"], preferred_element_type=jnp.float32)
    return h + matmul((jax.nn.silu(gate) * up).astype(jnp.bfloat16), w["w_down"])


def adamw(w, m, v, g):
    m = 0.9 * m + 0.1 * g
    v = 0.95 * v + 0.05 * g * g
    step = m * lax.rsqrt(v + 1e-8) + 0.1 * w
    return (w - 0.02 * step).astype(jnp.bfloat16), m, v


def stack(weights, h):
    return lax.scan(lambda h, w: (layer(h, w), None), h, weights)[0]


def reference(x, dy, w_gate, w_up, w_down, m_w_gate, m_w_up, m_w_down, v_w_gate, v_w_up, v_w_down):
    weights = dict(zip(NAMES, (w_gate, w_up, w_down), strict=True))

    def take(so_far, sequence):
        h, by_y = sequence
        _, back = jax.vjp(lambda w: stack(w, h), weights)
        return jax.tree.map(lambda total, term: total + term.astype(jnp.float32), so_far, back(by_y)[0]), None

    none_yet = {name: jnp.zeros(w.shape, jnp.float32) for name, w in weights.items()}
    by_weights, _ = lax.scan(take, none_yet, (x, dy))
    gradients = [by_weights[name].astype(jnp.bfloat16).astype(jnp.float32) for name in NAMES]
    new = [
        adamw(w.astype(jnp.float32), m, v, g)
        for w, m, v, g in zip((w_gate, w_up, w_down), (m_w_gate, m_w_up, m_w_down), (v_w_gate, v_w_up, v_w_down), gradients, strict=True)
    ]
    return tuple(one[which] for which in range(3) for one in new)
```

```python
import functools

import jax
import jax.numpy as jnp
from jax import lax
from jax.experimental import pallas as pl
from jax.experimental.pallas import tpu as pltpu
from jax.sharding import PartitionSpec as P

F32, BF16 = jnp.float32, jnp.bfloat16
MESH = pl.DeviceIdType.MESH
CHUNK = 512
AHEAD = 4


def adamw(w, m, v, g):
    m = 0.9 * m + 0.1 * g
    v = 0.95 * v + 0.05 * g * g
    step = m * lax.rsqrt(v + 1e-8) + 0.1 * w
    return (w - 0.02 * step).astype(jnp.bfloat16), m, v


def dot(a, b):
    return jnp.dot(a, b, preferred_element_type=F32)


def kernel(
    x_hbm, dy_hbm, pk_hbm, full_hbm, out_hbm,
    H, DY, A, AT, DYT, acc, act, dg, du, wt, wtT, G, R0, S1, own, R1, T2, R2, T3, R3, O,
    load_sem, wt_sem, ag_send, ag_recv, fw_send, fw_recv, send0, recv0, send1, recv1, send2, recv2, send3, recv3, out_sem,
):
    tokens, d_model = H.shape
    tiles = pk_hbm.shape[0]
    half = tiles // 2
    width = act.shape[1]
    chunks = tokens // CHUNK
    s, r = lax.axis_index("s"), lax.axis_index("r")
    core, chip = s % 2, s // 2
    partner = s + 1 - 2 * core
    chips = ((chip + 2) % 4, chip + 1 - 2 * (chip % 2), (chip + 2) % 4 + 1 - 2 * (chip % 2))
    peers = [2 * c + core for c in chips]
    near = r + 1 - 2 * (r % 2)
    far = (r + 2) % 4

    barrier = pltpu.get_barrier_semaphore()
    for where in [{"s": p} for p in [partner] + peers] + [{"r": near}, {"r": far}]:
        pl.semaphore_signal(barrier, inc=1, device_id=where, device_id_type=MESH)
    pl.semaphore_wait(barrier, 6)

    def remote(src, dst, send, recv, where):
        return pltpu.make_async_remote_copy(src_ref=src, dst_ref=dst, send_sem=send, recv_sem=recv, device_id=where, device_id_type=MESH)

    def shard(tile, n):
        where = (peers + [partner])[n]
        return remote(pk_hbm.at[tile], full_hbm.at[tile, chip, core], ag_send.at[tile, n], ag_recv.at[tile, n], {"s": where})

    def passed(tile, n):
        ref = full_hbm.at[tile, chips[n], core]
        return remote(ref, ref, fw_send.at[tile, n], fw_recv.at[tile, n], {"s": partner})

    def send_shard(tile):
        for n in range(4):
            shard(tile, n).start()

    def pass_on(tile):
        for n in range(3):
            shard(tile, n).wait_recv()
            passed(tile, n).start()

    def whole(tile):
        shard(tile, 3).wait_recv()
        for n in range(3):
            passed(tile, n).wait_recv()

    def load(tile, slot):
        pltpu.make_async_copy(pk_hbm.at[tile], wt.at[slot, chip, core], wt_sem.at[slot]).start()
        for n in range(1, 8):
            d = (s + n) % 8
            pltpu.make_async_copy(full_hbm.at[tile, d // 2, d % 2], wt.at[slot, d // 2, d % 2], wt_sem.at[slot]).start()

    def loaded(slot):
        pltpu.make_async_copy(full_hbm.at[0], wt.at[slot], wt_sem.at[slot]).wait()

    def weight(slot, which):
        return wt[slot, :, :, which].reshape(width, d_model)

    def rows(t):
        return pl.ds(pl.multiple_of(t * CHUNK, CHUNK), CHUNK)

    def each_chunk(body):
        lax.fori_loop(0, chunks, lambda t, _: (body(rows(t)), None)[1], None)

    def scale_of(wide):
        return lax.rsqrt(jnp.mean(wide * wide, -1, keepdims=True) + 1e-6)

    for tile in range(AHEAD):
        send_shard(tile)
    get_x = pltpu.make_async_copy(x_hbm, H, load_sem.at[0])
    get_dy = pltpu.make_async_copy(dy_hbm, DY, load_sem.at[1])
    get_x.start()
    get_dy.start()
    get_x.wait()

    def prepare_forward(at):
        wide = H[at].astype(F32)
        A[at] = (wide * scale_of(wide)).astype(BF16)
        acc[at] = jnp.zeros((CHUNK, d_model), F32)

    each_chunk(prepare_forward)
    pass_on(0)
    whole(0)
    load(0, 0)

    def forward(k, _):
        slot = k % 2
        send_shard(k + AHEAD)
        pass_on(k + 1)
        loaded(slot)

        def body(at):
            a = A[at]
            gate = dot(a, weight(slot, 0))
            up = dot(a, weight(slot, 1))
            sig = 0.5 * jnp.tanh(0.5 * gate) + 0.5
            acc[at] += dot((gate * sig * up).astype(BF16), weight(slot, 2))

        each_chunk(body)
        whole(k + 1)
        load(k + 1, 1 - slot)

    lax.fori_loop(0, half, forward, None)
    get_dy.wait()

    def prepare_last(at):
        h = (H[at].astype(F32) + acc[at].astype(BF16).astype(F32)).astype(BF16)
        H[at] = h
        wide = h.astype(F32)
        a = (wide * scale_of(wide)).astype(BF16)
        A[at] = a
        AT[:, at] = a.T
        DYT[:, at] = DY[at].T
        acc[at] = jnp.zeros((CHUNK, d_model), F32)

    each_chunk(prepare_last)

    def prepare_first(at):
        wide = H[at].astype(F32)
        scale = scale_of(wide)
        ct = acc[at].astype(BF16).astype(F32)
        by = ct * scale - wide * (jnp.sum(ct * wide, -1, keepdims=True) * (scale * scale * scale) * (1.0 / d_model))
        by = (DY[at].astype(F32) + by.astype(BF16).astype(F32)).astype(BF16)
        DY[at] = by
        DYT[:, at] = by.T

    def prepare_first_a(at):
        wide = H[at].astype(F32)
        a = (wide * scale_of(wide)).astype(BF16)
        A[at] = a
        AT[:, at] = a.T

    def stage0(i):
        slot = i % 2
        return remote(G.at[slot, :, 1 - core], R0.at[slot], send0, recv0.at[slot], {"s": partner})

    def stage1(i, n):
        slot = i % 2
        return remote(S1.at[chips[n]], R1.at[slot, n], send1.at[n], recv1.at[slot, n], {"s": peers[n]})

    def stage2(i):
        return remote(T2, R2.at[i % 2], send2, recv2.at[i % 2], {"r": near})

    def stage3(i):
        return remote(T3, R3.at[i % 2], send3, recv3.at[i % 2], {"r": far})

    def put(i):
        return pltpu.make_async_copy(O, out_hbm.at[i], out_sem)

    def when(i, lo, hi):
        return pl.when(jnp.logical_and(i >= lo, i < hi))

    def sums(q):
        def done(i, copies):
            @when(i, 1, tiles + 1)
            def _():
                for copy in copies(i - 1):
                    copy()

        i4 = q - 4
        done(i4, lambda i: [put(i).wait])

        @when(i4, 0, tiles)
        def _():
            stage3(i4).wait_recv()
            O[...] = (T3[...].astype(F32) + R3[i4 % 2].astype(F32)).astype(BF16)
            put(i4).start()

        i3 = q - 3
        done(i3, lambda i: [stage3(i).wait_send])

        @when(i3, 0, tiles)
        def _():
            stage2(i3).wait_recv()
            T3[...] = (T2[...].astype(F32) + R2[i3 % 2].astype(F32)).astype(BF16)
            stage3(i3).start()

        i2 = q - 2
        done(i2, lambda i: [stage2(i).wait_send])

        @when(i2, 0, tiles)
        def _():
            for n in range(3):
                stage1(i2, n).wait_recv()
            slot = i2 % 2
            T2[...] = (own[...] + R1[slot, 0].astype(F32) + R1[slot, 1].astype(F32) + R1[slot, 2].astype(F32)).astype(BF16)
            stage2(i2).start()

        i1 = q - 1
        done(i1, lambda i: [stage1(i, n).wait_send for n in range(3)])

        @when(i1, 0, tiles)
        def _():
            stage0(i1).wait()
            slot = i1 % 2
            own[...] = G[slot, chip, core].astype(F32) + R0[slot, chip].astype(F32)
            for c in range(4):
                S1[c] = (G[slot, c, core].astype(F32) + R0[slot, c].astype(F32)).astype(BF16)
            for n in range(3):
                stage1(i1, n).start()

        @when(q, 0, tiles)
        def _():
            stage0(q).start()

    def backward(q, _):
        slot = q % 2

        @pl.when(q == half)
        def _():
            each_chunk(prepare_first)
            again = pltpu.make_async_copy(x_hbm, H, load_sem.at[0])
            again.start()
            again.wait()
            each_chunk(prepare_first_a)

        @pl.when(q < half - AHEAD)
        def _():
            send_shard(q + half + AHEAD)

        @pl.when(q < half - 1)
        def _():
            pass_on(q + half + 1)

        @pl.when(q < tiles)
        def _():
            loaded(slot)
            for which in range(3):
                wtT[which] = weight(slot, which).T

            def body(at):
                a = A[at]
                gate = dot(a, weight(slot, 0))
                up = dot(a, weight(slot, 1))
                by = dot(DY[at], wtT[2]).astype(BF16).astype(F32)
                sig = 0.5 * jnp.tanh(0.5 * gate) + 0.5
                silu = gate * sig
                act[at] = (silu * up).astype(BF16)
                du[at] = (by * silu).astype(BF16)
                dg[at] = (by * up * (sig + silu * (1.0 - sig))).astype(BF16)

            each_chunk(body)

            @pl.when(q < half)
            def _():
                def body(at):
                    acc[at] += dot(dg[at], wtT[0]) + dot(du[at], wtT[1])

                each_chunk(body)

            def keep(which, value):
                G[slot, :, :, which] = value.reshape(4, 2, d_model // 8, width)

            keep(0, dot(AT[...], dg[...]).astype(BF16))
            keep(1, dot(AT[...], du[...]).astype(BF16))
            keep(2, dot(DYT[...], act[...]).astype(BF16).T)

        sums(q)

        @pl.when(q < half - 1)
        def _():
            whole(q + half + 1)
            load(q + half + 1, 1 - slot)

        @pl.when(jnp.logical_and(q >= half - 1, q < tiles - 1))
        def _():
            load(q - half + 1, 1 - slot)

    lax.fori_loop(0, tiles + 5, backward, None)

    def sent(tile, _):
        for n in range(4):
            shard(tile, n).wait_send()
        for n in range(3):
            passed(tile, n).wait_send()

    lax.fori_loop(0, tiles, sent, None)


def gradients_of(x, dy, packed):
    tiles, _, height, width = packed.shape
    tokens, d_model = x.shape
    piece = (3, height, width)
    vmem, sem = pltpu.VMEM, pltpu.SemaphoreType.DMA
    flops = 17 * 2 * tokens * d_model * width * tiles // 2
    _, out = pl.pallas_call(
        kernel,
        out_shape=(jax.ShapeDtypeStruct((tiles, 4, 2) + piece, BF16), jax.ShapeDtypeStruct((tiles,) + piece, BF16)),
        in_specs=[pl.BlockSpec(memory_space=pltpu.HBM)] * 3,
        out_specs=[pl.BlockSpec(memory_space=pltpu.HBM)] * 2,
        scratch_shapes=[
            vmem((tokens, d_model), BF16),
            vmem((tokens, d_model), BF16),
            vmem((tokens, d_model), BF16),
            vmem((d_model, tokens), BF16),
            vmem((d_model, tokens), BF16),
            vmem((tokens, d_model), F32),
            vmem((tokens, width), BF16),
            vmem((tokens, width), BF16),
            vmem((tokens, width), BF16),
            vmem((2, 4, 2) + piece, BF16),
            vmem((3, d_model, width), BF16),
            vmem((2, 4, 2) + piece, BF16),
            vmem((2, 4) + piece, BF16),
            vmem((4,) + piece, BF16),
            vmem(piece, F32),
            vmem((2, 3) + piece, BF16),
            vmem(piece, BF16),
            vmem((2,) + piece, BF16),
            vmem(piece, BF16),
            vmem((2,) + piece, BF16),
            vmem(piece, BF16),
            sem((2,)),
            sem((2,)),
            sem((tiles, 4)),
            sem((tiles, 4)),
            sem((tiles, 3)),
            sem((tiles, 3)),
            sem, sem((2,)),
            sem((3,)), sem((2, 3)),
            sem, sem((2,)),
            sem, sem((2,)),
            sem,
        ],
        compiler_params=pltpu.CompilerParams(collective_id=0, has_side_effects=True, vmem_limit_bytes=67043328),
        cost_estimate=pl.CostEstimate(flops=flops, bytes_accessed=64 << 20, transcendentals=0),
        name="step",
    )(x, dy, packed)
    return out


def solution(mesh):
    def pack(gate, up, down):
        rows, hidden = gate.shape

        def columns(w):
            return w.reshape(rows, 8, 8, hidden // 64).transpose(2, 0, 1, 3).reshape(8, rows, hidden // 8)

        return jnp.stack([columns(gate), columns(up), down.reshape(8, -1, down.shape[1])], 1)

    def unpack(tiles):
        def columns(t):
            j, rows, width = t.shape
            return t.reshape(j, rows, 8, width // 8).transpose(1, 2, 0, 3).reshape(rows, j * width)

        return columns(tiles[:, 0]), columns(tiles[:, 1]), tiles[:, 2].reshape(-1, tiles.shape[3])

    def step(x, dy, *arrays):
        weights, m, v = (arrays[i : i + 3] for i in (0, 3, 6))
        layers = weights[0].shape[0]
        packed = jnp.concatenate([pack(*(w[number] for w in weights)) for number in range(layers)])
        out = gradients_of(x[0], dy[0], packed)
        half = out.shape[0] // 2
        mine = [unpack(out[half:]), unpack(out[:half])]
        gradients = [jnp.stack([mine[number][i] for number in range(layers)]).astype(jnp.float32) for i in range(3)]
        new = [adamw(w.astype(jnp.float32), m, v, g) for w, m, v, g in zip(weights, m, v, gradients, strict=True)]
        return tuple(one[which] for which in range(3) for one in new)

    states, cut = P(("rep", "r", "s"), None, None), P(None, "s", None)
    return jax.shard_map(
        step,
        mesh=mesh,
        in_specs=(states, states) + (cut,) * 9,
        out_specs=(P("rep", "s", None),) * 9,
        check_vma=False,
    )
```

```python
import functools

import jax
import jax.numpy as jnp
from jax import lax
from jax.experimental import pallas as pl
from jax.experimental.pallas import tpu as pltpu
from jax.sharding import PartitionSpec as P

F32, BF16 = jnp.float32, jnp.bfloat16
MESH = pl.DeviceIdType.MESH
CHUNK = 512
AHEAD = 4


def adamw(w, m, v, g):
    m = 0.9 * m + 0.1 * g
    v = 0.95 * v + 0.05 * g * g
    step = m * lax.rsqrt(v + 1e-8) + 0.1 * w
    return (w - 0.02 * step).astype(jnp.bfloat16), m, v


def dot(a, b):
    return jnp.dot(a, b, preferred_element_type=F32)


def kernel(
    x_hbm, dy_hbm, pk_hbm, full_hbm, out_hbm,
    H, DY, A, AT, DYT, acc, act0, act1, dg0, dg1, du0, du1, wt, wtT, G, R0, S1, own, R1, T2, R2, T3, R3, O,
    load_sem, wt_sem, ag_send, ag_recv, fw_send, fw_recv, send0, recv0, send1, recv1, send2, recv2, send3, recv3, out_sem,
):
    tokens, d_model = H.shape
    tiles = pk_hbm.shape[0]
    half = tiles // 2
    width = act0.shape[1]
    act, dg, du = (act0, act1), (dg0, dg1), (du0, du1)
    chunks = tokens // CHUNK
    s, r = lax.axis_index("s"), lax.axis_index("r")
    core, chip = s % 2, s // 2
    partner = s + 1 - 2 * core
    chips = ((chip + 2) % 4, chip + 1 - 2 * (chip % 2), (chip + 2) % 4 + 1 - 2 * (chip % 2))
    peers = [2 * c + core for c in chips]
    near = r + 1 - 2 * (r % 2)
    far = (r + 2) % 4

    barrier = pltpu.get_barrier_semaphore()
    for where in [{"s": p} for p in [partner] + peers] + [{"r": near}, {"r": far}]:
        pl.semaphore_signal(barrier, inc=1, device_id=where, device_id_type=MESH)
    pl.semaphore_wait(barrier, 6)

    def remote(src, dst, send, recv, where):
        return pltpu.make_async_remote_copy(src_ref=src, dst_ref=dst, send_sem=send, recv_sem=recv, device_id=where, device_id_type=MESH)

    def shard(tile, n):
        where = (peers + [partner])[n]
        return remote(pk_hbm.at[tile], full_hbm.at[tile, chip, core], ag_send.at[tile, n], ag_recv.at[tile, n], {"s": where})

    def passed(tile, n):
        ref = full_hbm.at[tile, chips[n], core]
        return remote(ref, ref, fw_send.at[tile, n], fw_recv.at[tile, n], {"s": partner})

    def send_shard(tile):
        for n in range(4):
            shard(tile, n).start()

    def pass_on(tile):
        for n in range(3):
            shard(tile, n).wait_recv()
            passed(tile, n).start()

    def whole(tile):
        shard(tile, 3).wait_recv()
        for n in range(3):
            passed(tile, n).wait_recv()

    def load(tile, slot):
        pltpu.make_async_copy(pk_hbm.at[tile], wt.at[slot, chip, core], wt_sem.at[slot]).start()
        for n in range(1, 8):
            d = (s + n) % 8
            pltpu.make_async_copy(full_hbm.at[tile, d // 2, d % 2], wt.at[slot, d // 2, d % 2], wt_sem.at[slot]).start()

    def loaded(slot):
        pltpu.make_async_copy(full_hbm.at[0], wt.at[slot], wt_sem.at[slot]).wait()

    def weight(slot, which):
        return wt[slot, :, :, which].reshape(width, d_model)

    def rows(t):
        return pl.ds(pl.multiple_of(t * CHUNK, CHUNK), CHUNK)

    def each_chunk(body):
        lax.fori_loop(0, chunks, lambda t, _: (body(rows(t), column(t)), None)[1], None)

    def column(t):
        return pl.ds(pl.multiple_of(t // 2 * CHUNK + t % 2 * (tokens // 2), CHUNK), CHUNK)

    def each_pair(body, between=None):
        def pair(p, _):
            body(p, [rows(2 * p), rows(2 * p + 1)])
            if between is not None:
                pl.when(p == chunks // 4)(between)

        lax.fori_loop(0, chunks // 2, pair, None)

    def scale_of(wide):
        return lax.rsqrt(jnp.mean(wide * wide, -1, keepdims=True) + 1e-6)

    for tile in range(AHEAD):
        send_shard(tile)
    get_x = pltpu.make_async_copy(x_hbm, H, load_sem.at[0])
    get_dy = pltpu.make_async_copy(dy_hbm, DY, load_sem.at[1])
    get_x.start()
    get_dy.start()
    get_x.wait()

    def prepare_forward(at, to):
        wide = H[at].astype(F32)
        A[at] = (wide * scale_of(wide)).astype(BF16)
        acc[at] = jnp.zeros((CHUNK, d_model), F32)

    each_chunk(prepare_forward)
    pass_on(0)
    whole(0)
    load(0, 0)

    def forward(k, _):
        slot = k % 2
        send_shard(k + AHEAD)
        loaded(slot)

        def body(p, both):
            for at in both:
                a = A[at]
                gate = dot(a, weight(slot, 0))
                up = dot(a, weight(slot, 1))
                sig = 0.5 * jnp.tanh(0.5 * gate) + 0.5
                acc[at] += dot((gate * sig * up).astype(BF16), weight(slot, 2))

        each_pair(body, lambda: pass_on(k + 1))
        whole(k + 1)
        load(k + 1, 1 - slot)

    lax.fori_loop(0, half, forward, None)
    pass_on(half + 1)
    get_dy.wait()

    def prepare_last(at, to):
        h = (H[at].astype(F32) + acc[at].astype(BF16).astype(F32)).astype(BF16)
        H[at] = h
        wide = h.astype(F32)
        a = (wide * scale_of(wide)).astype(BF16)
        A[at] = a
        AT[:, to] = a.T
        DYT[:, to] = DY[at].T
        acc[at] = jnp.zeros((CHUNK, d_model), F32)

    each_chunk(prepare_last)

    def prepare_first(at, to):
        wide = H[at].astype(F32)
        scale = scale_of(wide)
        ct = acc[at].astype(BF16).astype(F32)
        by = ct * scale - wide * (jnp.sum(ct * wide, -1, keepdims=True) * (scale * scale * scale) * (1.0 / d_model))
        by = (DY[at].astype(F32) + by.astype(BF16).astype(F32)).astype(BF16)
        DY[at] = by
        DYT[:, to] = by.T

    def prepare_first_a(at, to):
        wide = H[at].astype(F32)
        a = (wide * scale_of(wide)).astype(BF16)
        A[at] = a
        AT[:, to] = a.T

    def stage0(i):
        slot = i % 2
        return remote(G.at[slot, :, 1 - core], R0.at[slot], send0, recv0.at[slot], {"s": partner})

    def stage1(i, n):
        slot = i % 2
        return remote(S1.at[chips[n]], R1.at[slot, n], send1.at[n], recv1.at[slot, n], {"s": peers[n]})

    def stage2(i):
        return remote(T2, R2.at[i % 2], send2, recv2.at[i % 2], {"r": near})

    def stage3(i):
        return remote(T3, R3.at[i % 2], send3, recv3.at[i % 2], {"r": far})

    def put(i):
        return pltpu.make_async_copy(O, out_hbm.at[i], out_sem)

    def when(i, lo, hi):
        return pl.when(jnp.logical_and(i >= lo, i < hi))

    def sums(q):
        def done(i, copies):
            @when(i, 1, tiles + 1)
            def _():
                for copy in copies(i - 1):
                    copy()

        i4 = q - 4
        done(i4, lambda i: [put(i).wait])

        @when(i4, 0, tiles)
        def _():
            stage3(i4).wait_recv()
            O[...] = (T3[...].astype(F32) + R3[i4 % 2].astype(F32)).astype(BF16)
            put(i4).start()

        i3 = q - 3
        done(i3, lambda i: [stage3(i).wait_send])

        @when(i3, 0, tiles)
        def _():
            stage2(i3).wait_recv()
            T3[...] = (T2[...].astype(F32) + R2[i3 % 2].astype(F32)).astype(BF16)
            stage3(i3).start()

        i2 = q - 2
        done(i2, lambda i: [stage2(i).wait_send])

        @when(i2, 0, tiles)
        def _():
            for n in range(3):
                stage1(i2, n).wait_recv()
            slot = i2 % 2
            T2[...] = (own[...] + R1[slot, 0].astype(F32) + R1[slot, 1].astype(F32) + R1[slot, 2].astype(F32)).astype(BF16)
            stage2(i2).start()

        i1 = q - 1
        done(i1, lambda i: [stage1(i, n).wait_send for n in range(3)])

        @when(i1, 0, tiles)
        def _():
            stage0(i1).wait()
            slot = i1 % 2
            own[...] = G[slot, chip, core].astype(F32) + R0[slot, chip].astype(F32)
            for c in range(4):
                S1[c] = (G[slot, c, core].astype(F32) + R0[slot, c].astype(F32)).astype(BF16)
            for n in range(3):
                stage1(i1, n).start()

        @when(q, 0, tiles)
        def _():
            stage0(q).start()

    def backward(q, _):
        slot = q % 2

        @pl.when(q == half)
        def _():
            each_chunk(prepare_first)
            again = pltpu.make_async_copy(x_hbm, H, load_sem.at[0])
            again.start()
            again.wait()
            each_chunk(prepare_first_a)

        @pl.when(q < half - AHEAD)
        def _():
            send_shard(q + half + AHEAD)

        @pl.when(q < tiles)
        def _():
            loaded(slot)
            for which in range(3):
                wtT[which] = weight(slot, which).T

            def front(p, both):
                for n, at in enumerate(both):
                    a = A[at]
                    gate = dot(a, weight(slot, 0))
                    up = dot(a, weight(slot, 1))
                    by = dot(DY[at], wtT[2]).astype(BF16).astype(F32)
                    sig = 0.5 * jnp.tanh(0.5 * gate) + 0.5
                    silu = gate * sig
                    act[n][rows(p)] = (silu * up).astype(BF16)
                    du[n][rows(p)] = (by * silu).astype(BF16)
                    dg[n][rows(p)] = (by * up * (sig + silu * (1.0 - sig))).astype(BF16)

            def both_ways(p, both):
                front(p, both)
                for n, at in enumerate(both):
                    acc[at] += dot(dg[n][rows(p)], wtT[0]) + dot(du[n][rows(p)], wtT[1])

            @pl.when(q < half)
            def _():
                each_pair(both_ways)

            @pl.when(q >= half)
            def _():
                each_pair(front)

            @pl.when(q < half - 2)
            def _():
                pass_on(q + half + 2)

            @pl.when(q < half - 1)
            def _():
                whole(q + half + 1)
                load(q + half + 1, 1 - slot)

            @pl.when(jnp.logical_and(q >= half - 1, q < tiles - 1))
            def _():
                load(q - half + 1, 1 - slot)

            def over_tokens(left, right):
                cut = tokens // 2
                return dot(left[:, :cut], right[0][...]) + dot(left[:, cut:], right[1][...])

            def keep(which, value):
                G[slot, :, :, which] = value.reshape(4, 2, d_model // 8, width)

            keep(0, over_tokens(AT, dg).astype(BF16))
            keep(1, over_tokens(AT, du).astype(BF16))
            keep(2, over_tokens(DYT, act).astype(BF16).T)

        sums(q)

    lax.fori_loop(0, tiles + 5, backward, None)

    def sent(tile, _):
        for n in range(4):
            shard(tile, n).wait_send()
        for n in range(3):
            passed(tile, n).wait_send()

    lax.fori_loop(0, tiles, sent, None)


def gradients_of(x, dy, packed):
    tiles, _, height, width = packed.shape
    tokens, d_model = x.shape
    piece = (3, height, width)
    vmem, sem = pltpu.VMEM, pltpu.SemaphoreType.DMA
    flops = 17 * 2 * tokens * d_model * width * tiles // 2
    _, out = pl.pallas_call(
        kernel,
        out_shape=(jax.ShapeDtypeStruct((tiles, 4, 2) + piece, BF16), jax.ShapeDtypeStruct((tiles,) + piece, BF16)),
        in_specs=[pl.BlockSpec(memory_space=pltpu.HBM)] * 3,
        out_specs=[pl.BlockSpec(memory_space=pltpu.HBM)] * 2,
        scratch_shapes=[
            vmem((tokens, d_model), BF16),
            vmem((tokens, d_model), BF16),
            vmem((tokens, d_model), BF16),
            vmem((d_model, tokens), BF16),
            vmem((d_model, tokens), BF16),
            vmem((tokens, d_model), F32),
            *[vmem((tokens // 2, width), BF16)] * 6,
            vmem((2, 4, 2) + piece, BF16),
            vmem((3, d_model, width), BF16),
            vmem((2, 4, 2) + piece, BF16),
            vmem((2, 4) + piece, BF16),
            vmem((4,) + piece, BF16),
            vmem(piece, F32),
            vmem((2, 3) + piece, BF16),
            vmem(piece, BF16),
            vmem((2,) + piece, BF16),
            vmem(piece, BF16),
            vmem((2,) + piece, BF16),
            vmem(piece, BF16),
            sem((2,)),
            sem((2,)),
            sem((tiles, 4)),
            sem((tiles, 4)),
            sem((tiles, 3)),
            sem((tiles, 3)),
            sem, sem((2,)),
            sem((3,)), sem((2, 3)),
            sem, sem((2,)),
            sem, sem((2,)),
            sem,
        ],
        compiler_params=pltpu.CompilerParams(collective_id=0, has_side_effects=True, vmem_limit_bytes=67043328),
        cost_estimate=pl.CostEstimate(flops=flops, bytes_accessed=64 << 20, transcendentals=0),
        name="step",
    )(x, dy, packed)
    return out


def swapped(t):
    return pltpu.roll(t, 64, 1)


def woven(left, right, odd):
    low = lax.broadcasted_iota(jnp.int32, left.shape, 1) < 64
    return jnp.where(low, swapped(left), right) if odd else jnp.where(low, left, swapped(right))


def lanes(n):
    return slice(128 * n, 128 * (n + 1))


def pack_kernel(gate, up, down, out):
    for which, ref in enumerate((gate, up)):
        for p in range(4):
            for e in range(4):
                left, right = (ref[0, :, lanes(4 * d + p)].astype(F32) for d in (2 * e, 2 * e + 1))
                for odd in range(2):
                    out[2 * p + odd, which, :, lanes(e)] = woven(left, right, odd).astype(BF16)
    for j in range(8):
        out[j, 2] = down[0, j]


def adamw_kernel(g, *refs):
    ins, outs = refs[:9], refs[9:]

    def update(which, at, gradient):
        new = adamw(ins[which][at].astype(F32), ins[3 + which][at], ins[6 + which][at], gradient)
        for k in range(3):
            outs[3 * k + which][at] = new[k]

    for which in range(2):
        for p in range(4):
            for e in range(4):
                left, right = (g[2 * p + odd, which, :, lanes(e)].astype(F32) for odd in range(2))
                for odd in range(2):
                    update(which, (0, slice(None), lanes(4 * (2 * e + odd) + p)), woven(left, right, odd))
    for j in range(8):
        update(2, (0, j), g[j, 2].astype(F32))


def solution(mesh):
    def step(x, dy, *arrays):
        layers, height, hidden = arrays[0].shape
        d_model = arrays[2].shape[2]
        rows = 16

        def tiled(w):
            return w.reshape(layers, 8, height, d_model)

        arrays = [tiled(w) if n % 3 == 2 else w for n, w in enumerate(arrays)]
        wide = pl.BlockSpec((1, rows, hidden), lambda l, n: (l, n, 0))
        tall = pl.BlockSpec((1, 8, rows, d_model), lambda l, n: (l, 0, n, 0))
        each = [wide, wide, tall]
        grid = (layers, height // rows)
        tiles = (8, 3, rows, hidden // 8)
        packed = pl.pallas_call(
            pack_kernel,
            out_shape=jax.ShapeDtypeStruct((8 * layers, 3, height, hidden // 8), BF16),
            grid=grid,
            in_specs=each,
            out_specs=pl.BlockSpec(tiles, lambda l, n: (l, 0, n, 0)),
            name="pack",
        )(*arrays[:3])
        out = gradients_of(x[0], dy[0], packed)
        new = pl.pallas_call(
            adamw_kernel,
            out_shape=[jax.ShapeDtypeStruct(a.shape, a.dtype) for a in arrays],
            grid=grid,
            in_specs=[pl.BlockSpec(tiles, lambda l, n: (layers - 1 - l, 0, n, 0))] + each * 3,
            out_specs=each * 3,
            name="adamw",
        )(out, *arrays)
        return tuple(w.reshape(layers, 8 * height, d_model) if n % 3 == 2 else w for n, w in enumerate(new))

    states, cut = P(("rep", "r", "s"), None, None), P(None, "s", None)
    return jax.shard_map(
        step,
        mesh=mesh,
        in_specs=(states, states) + (cut,) * 9,
        out_specs=(P("rep", "s", None),) * 9,
        check_vma=False,
    )
```

```python
import functools

import jax
import jax.numpy as jnp
from jax import lax
from jax.experimental import pallas as pl
from jax.experimental.pallas import tpu as pltpu
from jax.sharding import PartitionSpec as P

F32, BF16 = jnp.float32, jnp.bfloat16
MESH = pl.DeviceIdType.MESH
CHUNK = 512
AHEAD = 4


def adamw(w, m, v, g):
    m = 0.9 * m + 0.1 * g
    v = 0.95 * v + 0.05 * g * g
    step = m * lax.rsqrt(v + 1e-8) + 0.1 * w
    return (w - 0.02 * step).astype(jnp.bfloat16), m, v


def dot(a, b):
    return jnp.dot(a, b, preferred_element_type=F32)


def kernel(
    x_hbm, dy_hbm, pk_hbm, full_hbm, out_hbm,
    H, DY, A, AT, DYT, acc, act0, act1, dg0, dg1, du0, du1, wt, wtT, G, R0, S1, own, R1, T2, R2, T3, R3, O,
    load_sem, wt_sem, ag_send, ag_recv, fw_send, fw_recv, send0, recv0, send1, recv1, send2, recv2, send3, recv3, out_sem,
):
    tokens, d_model = H.shape
    tiles = pk_hbm.shape[0]
    half = tiles // 2
    width = act0.shape[1]
    act, dg, du = (act0, act1), (dg0, dg1), (du0, du1)
    chunks = tokens // CHUNK
    s, r = lax.axis_index("s"), lax.axis_index("r")
    core, chip = s % 2, s // 2
    partner = s + 1 - 2 * core
    chips = ((chip + 2) % 4, chip + 1 - 2 * (chip % 2), (chip + 2) % 4 + 1 - 2 * (chip % 2))
    peers = [2 * c + core for c in chips]
    near = r + 1 - 2 * (r % 2)
    far = (r + 2) % 4

    barrier = pltpu.get_barrier_semaphore()
    for where in [{"s": p} for p in [partner] + peers] + [{"r": near}, {"r": far}]:
        pl.semaphore_signal(barrier, inc=1, device_id=where, device_id_type=MESH)
    pl.semaphore_wait(barrier, 6)

    def remote(src, dst, send, recv, where):
        return pltpu.make_async_remote_copy(src_ref=src, dst_ref=dst, send_sem=send, recv_sem=recv, device_id=where, device_id_type=MESH)

    def shard(tile, n):
        where = (peers + [partner])[n]
        return remote(pk_hbm.at[tile], full_hbm.at[tile, chip, core], ag_send.at[tile, n], ag_recv.at[tile, n], {"s": where})

    def passed(tile, n):
        ref = full_hbm.at[tile, chips[n], core]
        return remote(ref, ref, fw_send.at[tile, n], fw_recv.at[tile, n], {"s": partner})

    def send_shard(tile):
        for n in range(4):
            shard(tile, n).start()

    def pass_on(tile):
        for n in range(3):
            shard(tile, n).wait_recv()
            passed(tile, n).start()

    def whole(tile):
        shard(tile, 3).wait_recv()
        for n in range(3):
            passed(tile, n).wait_recv()

    def load(tile, slot):
        pltpu.make_async_copy(pk_hbm.at[tile], wt.at[slot, chip, core], wt_sem.at[slot]).start()
        for n in range(1, 8):
            d = (s + n) % 8
            pltpu.make_async_copy(full_hbm.at[tile, d // 2, d % 2], wt.at[slot, d // 2, d % 2], wt_sem.at[slot]).start()

    def loaded(slot):
        pltpu.make_async_copy(full_hbm.at[0], wt.at[slot], wt_sem.at[slot]).wait()

    def weight(slot, which):
        return wt[slot, :, :, which].reshape(width, d_model)

    def rows(t):
        return pl.ds(pl.multiple_of(t * CHUNK, CHUNK), CHUNK)

    def each_chunk(body):
        lax.fori_loop(0, chunks, lambda t, _: (body(rows(t), column(t)), None)[1], None)

    def column(t):
        return pl.ds(pl.multiple_of(t // 2 * CHUNK + t % 2 * (tokens // 2), CHUNK), CHUNK)

    def each_pair(body, between=None):
        def pair(p, _):
            body(p, [rows(2 * p), rows(2 * p + 1)])
            if between is not None:
                pl.when(p == chunks // 4)(between)

        lax.fori_loop(0, chunks // 2, pair, None)

    def scale_of(wide):
        return lax.rsqrt(jnp.mean(wide * wide, -1, keepdims=True) + 1e-6)

    for tile in range(AHEAD):
        send_shard(tile)
    get_x = pltpu.make_async_copy(x_hbm, H, load_sem.at[0])
    get_dy = pltpu.make_async_copy(dy_hbm, DY, load_sem.at[1])
    get_x.start()
    get_dy.start()
    get_x.wait()

    def prepare_forward(at, to):
        wide = H[at].astype(F32)
        A[at] = (wide * scale_of(wide)).astype(BF16)
        acc[at] = jnp.zeros((CHUNK, d_model), F32)

    each_chunk(prepare_forward)
    get_dy.wait()

    def turn(at, to):
        DYT[:, to] = DY[at].T

    each_chunk(turn)
    pass_on(0)
    whole(0)
    load(0, 0)

    def forward(k, _):
        slot = k % 2
        send_shard(k + AHEAD)
        loaded(slot)

        def body(p, both):
            for at in both:
                a = A[at]
                gate = dot(a, weight(slot, 0))
                up = dot(a, weight(slot, 1))
                sig = 0.5 * jnp.tanh(0.5 * gate) + 0.5
                acc[at] += dot((gate * sig * up).astype(BF16), weight(slot, 2))

        each_pair(body, lambda: pass_on(k + 1))
        whole(k + 1)
        load(k + 1, 1 - slot)

    lax.fori_loop(0, half, forward, None)
    pass_on(half + 1)

    def prepare_last(at, to):
        h = (H[at].astype(F32) + acc[at].astype(BF16).astype(F32)).astype(BF16)
        H[at] = h
        wide = h.astype(F32)
        a = (wide * scale_of(wide)).astype(BF16)
        A[at] = a
        AT[:, to] = a.T
        acc[at] = jnp.zeros((CHUNK, d_model), F32)

    each_chunk(prepare_last)

    def prepare_first(at, to):
        wide = H[at].astype(F32)
        scale = scale_of(wide)
        ct = acc[at].astype(BF16).astype(F32)
        by = ct * scale - wide * (jnp.sum(ct * wide, -1, keepdims=True) * (scale * scale * scale) * (1.0 / d_model))
        by = (DY[at].astype(F32) + by.astype(BF16).astype(F32)).astype(BF16)
        DY[at] = by
        DYT[:, to] = by.T

    def prepare_first_a(at, to):
        wide = H[at].astype(F32)
        a = (wide * scale_of(wide)).astype(BF16)
        A[at] = a
        AT[:, to] = a.T

    def stage0(i):
        slot = i % 2
        return remote(G.at[slot, :, 1 - core], R0.at[slot], send0, recv0.at[slot], {"s": partner})

    def stage1(i, n):
        slot = i % 2
        return remote(S1.at[chips[n]], R1.at[slot, n], send1.at[n], recv1.at[slot, n], {"s": peers[n]})

    def stage2(i):
        return remote(T2, R2.at[i % 2], send2, recv2.at[i % 2], {"r": near})

    def stage3(i):
        return remote(T3, R3.at[i % 2], send3, recv3.at[i % 2], {"r": far})

    def put(i):
        return pltpu.make_async_copy(O, out_hbm.at[i], out_sem)

    def when(i, lo, hi):
        return pl.when(jnp.logical_and(i >= lo, i < hi))

    def sums(q):
        def done(i, copies):
            @when(i, 1, tiles + 1)
            def _():
                for copy in copies(i - 1):
                    copy()

        i4 = q - 4
        done(i4, lambda i: [put(i).wait])

        @when(i4, 0, tiles)
        def _():
            stage3(i4).wait_recv()
            O[...] = (T3[...].astype(F32) + R3[i4 % 2].astype(F32)).astype(BF16)
            put(i4).start()

        i3 = q - 3
        done(i3, lambda i: [stage3(i).wait_send])

        @when(i3, 0, tiles)
        def _():
            stage2(i3).wait_recv()
            T3[...] = (T2[...].astype(F32) + R2[i3 % 2].astype(F32)).astype(BF16)
            stage3(i3).start()

        i2 = q - 2
        done(i2, lambda i: [stage2(i).wait_send])

        @when(i2, 0, tiles)
        def _():
            for n in range(3):
                stage1(i2, n).wait_recv()
            slot = i2 % 2
            T2[...] = (own[...] + R1[slot, 0].astype(F32) + R1[slot, 1].astype(F32) + R1[slot, 2].astype(F32)).astype(BF16)
            stage2(i2).start()

        i1 = q - 1
        done(i1, lambda i: [stage1(i, n).wait_send for n in range(3)])

        @when(i1, 0, tiles)
        def _():
            stage0(i1).wait()
            slot = i1 % 2
            own[...] = G[slot, chip, core].astype(F32) + R0[slot, chip].astype(F32)
            for c in range(4):
                S1[c] = (G[slot, c, core].astype(F32) + R0[slot, c].astype(F32)).astype(BF16)
            for n in range(3):
                stage1(i1, n).start()

        @when(q, 0, tiles)
        def _():
            stage0(q).start()

    def backward(q, _):
        slot = q % 2

        @pl.when(q == half)
        def _():
            each_chunk(prepare_first)
            again = pltpu.make_async_copy(x_hbm, H, load_sem.at[0])
            again.start()
            again.wait()
            each_chunk(prepare_first_a)

        @pl.when(q < half - AHEAD)
        def _():
            send_shard(q + half + AHEAD)

        @pl.when(q < tiles)
        def _():
            loaded(slot)
            for which in range(3):
                wtT[which] = weight(slot, which).T

            def front(p, both):
                for n, at in enumerate(both):
                    a = A[at]
                    gate = dot(a, weight(slot, 0))
                    up = dot(a, weight(slot, 1))
                    by = dot(DY[at], wtT[2]).astype(BF16).astype(F32)
                    sig = 0.5 * jnp.tanh(0.5 * gate) + 0.5
                    silu = gate * sig
                    act[n][rows(p)] = (silu * up).astype(BF16)
                    du[n][rows(p)] = (by * silu).astype(BF16)
                    dg[n][rows(p)] = (by * up * (sig + silu * (1.0 - sig))).astype(BF16)

            def both_ways(p, both):
                front(p, both)
                for n, at in enumerate(both):
                    acc[at] += dot(dg[n][rows(p)], wtT[0]) + dot(du[n][rows(p)], wtT[1])

            @pl.when(q < half)
            def _():
                each_pair(both_ways)

            @pl.when(q >= half)
            def _():
                each_pair(front)

            @pl.when(q < half - 2)
            def _():
                pass_on(q + half + 2)

            @pl.when(q < half - 1)
            def _():
                whole(q + half + 1)
                load(q + half + 1, 1 - slot)

            @pl.when(jnp.logical_and(q >= half - 1, q < tiles - 1))
            def _():
                load(q - half + 1, 1 - slot)

            def over_tokens(left, right):
                cut = tokens // 2
                return dot(left[:, :cut], right[0][...]) + dot(left[:, cut:], right[1][...])

            def keep(which, value):
                G[slot, :, :, which] = value.reshape(4, 2, d_model // 8, width)

            keep(0, over_tokens(AT, dg).astype(BF16))
            keep(1, over_tokens(AT, du).astype(BF16))
            keep(2, over_tokens(DYT, act).astype(BF16).T)

        sums(q)

    lax.fori_loop(0, tiles + 5, backward, None)

    def sent(tile, _):
        for n in range(4):
            shard(tile, n).wait_send()
        for n in range(3):
            passed(tile, n).wait_send()

    lax.fori_loop(0, tiles, sent, None)


def gradients_of(x, dy, packed):
    tiles, _, height, width = packed.shape
    tokens, d_model = x.shape
    piece = (3, height, width)
    vmem, sem = pltpu.VMEM, pltpu.SemaphoreType.DMA
    flops = 17 * 2 * tokens * d_model * width * tiles // 2
    _, out = pl.pallas_call(
        kernel,
        out_shape=(jax.ShapeDtypeStruct((tiles, 4, 2) + piece, BF16), jax.ShapeDtypeStruct((tiles,) + piece, BF16)),
        in_specs=[pl.BlockSpec(memory_space=pltpu.HBM)] * 3,
        out_specs=[pl.BlockSpec(memory_space=pltpu.HBM)] * 2,
        scratch_shapes=[
            vmem((tokens, d_model), BF16),
            vmem((tokens, d_model), BF16),
            vmem((tokens, d_model), BF16),
            vmem((d_model, tokens), BF16),
            vmem((d_model, tokens), BF16),
            vmem((tokens, d_model), F32),
            *[vmem((tokens // 2, width), BF16)] * 6,
            vmem((2, 4, 2) + piece, BF16),
            vmem((3, d_model, width), BF16),
            vmem((2, 4, 2) + piece, BF16),
            vmem((2, 4) + piece, BF16),
            vmem((4,) + piece, BF16),
            vmem(piece, F32),
            vmem((2, 3) + piece, BF16),
            vmem(piece, BF16),
            vmem((2,) + piece, BF16),
            vmem(piece, BF16),
            vmem((2,) + piece, BF16),
            vmem(piece, BF16),
            sem((2,)),
            sem((2,)),
            sem((tiles, 4)),
            sem((tiles, 4)),
            sem((tiles, 3)),
            sem((tiles, 3)),
            sem, sem((2,)),
            sem((3,)), sem((2, 3)),
            sem, sem((2,)),
            sem, sem((2,)),
            sem,
        ],
        compiler_params=pltpu.CompilerParams(collective_id=0, has_side_effects=True, vmem_limit_bytes=67043328),
        cost_estimate=pl.CostEstimate(flops=flops, bytes_accessed=64 << 20, transcendentals=0),
        name="step",
    )(x, dy, packed)
    return out


def swapped(t):
    return pltpu.roll(t, 64, 1)


def woven(left, right, odd):
    low = lax.broadcasted_iota(jnp.int32, left.shape, 1) < 64
    return jnp.where(low, swapped(left), right) if odd else jnp.where(low, left, swapped(right))


def lanes(n):
    return slice(128 * n, 128 * (n + 1))


def pack_kernel(gate, up, down, out):
    for which, ref in enumerate((gate, up)):
        for p in range(4):
            for e in range(4):
                left, right = (ref[0, :, lanes(4 * d + p)].astype(F32) for d in (2 * e, 2 * e + 1))
                for odd in range(2):
                    out[2 * p + odd, which, :, lanes(e)] = woven(left, right, odd).astype(BF16)
    for j in range(8):
        out[j, 2] = down[0, j]


def adamw_kernel(g, *refs):
    ins, outs = refs[:9], refs[9:]

    def update(which, at, gradient):
        new = adamw(ins[which][at].astype(F32), ins[3 + which][at], ins[6 + which][at], gradient)
        for k in range(3):
            outs[3 * k + which][at] = new[k]

    for which in range(2):
        for p in range(4):
            for e in range(4):
                left, right = (g[2 * p + odd, which, :, lanes(e)].astype(F32) for odd in range(2))
                for odd in range(2):
                    update(which, (0, slice(None), lanes(4 * (2 * e + odd) + p)), woven(left, right, odd))
    for j in range(8):
        update(2, (0, j), g[j, 2].astype(F32))


def solution(mesh):
    def step(x, dy, *arrays):
        layers, height, hidden = arrays[0].shape
        d_model = arrays[2].shape[2]
        rows = 32

        def tiled(w):
            return w.reshape(layers, 8, height, d_model)

        arrays = [tiled(w) if n % 3 == 2 else w for n, w in enumerate(arrays)]
        wide = pl.BlockSpec((1, rows, hidden), lambda l, n: (l, n, 0))
        tall = pl.BlockSpec((1, 8, rows, d_model), lambda l, n: (l, 0, n, 0))
        each = [wide, wide, tall]
        grid = (layers, height // rows)
        tiles = (8, 3, rows, hidden // 8)
        packed = pl.pallas_call(
            pack_kernel,
            out_shape=jax.ShapeDtypeStruct((8 * layers, 3, height, hidden // 8), BF16),
            grid=grid,
            in_specs=each,
            out_specs=pl.BlockSpec(tiles, lambda l, n: (l, 0, n, 0)),
            name="pack",
        )(*arrays[:3])
        out = gradients_of(x[0], dy[0], packed)
        new = pl.pallas_call(
            adamw_kernel,
            out_shape=[jax.ShapeDtypeStruct(a.shape, a.dtype) for a in arrays],
            grid=grid,
            in_specs=[pl.BlockSpec(tiles, lambda l, n: (layers - 1 - l, 0, n, 0))] + each * 3,
            out_specs=each * 3,
            name="adamw",
        )(out, *arrays)
        return tuple(w.reshape(layers, 8 * height, d_model) if n % 3 == 2 else w for n, w in enumerate(new))

    states, cut = P(("rep", "r", "s"), None, None), P(None, "s", None)
    return jax.shard_map(
        step,
        mesh=mesh,
        in_specs=(states, states) + (cut,) * 9,
        out_specs=(P("rep", "s", None),) * 9,
        check_vma=False,
    )
```
